32 devices in a mesh: lat: 4 (over x, core), lon: 8 (over z, y).
Axes of the slice: x: 2, y: 2, z: 4, core: 2. Of those that a mesh axis runs over, the one named last changes fastest.
Arguments:
- tracers: bfloat16 [256, 1024, 32, 4], P('lat', 'lon'), may hold values from 0 to 2
- weights: bfloat16 [256, 8, 8, 128, 128], P('lat', 'lon'), may hold values from -1 to 1, as said below
- source_row: int32 [256, 8, 8], P('lat', 'lon'), may hold values from 0 to 255, as said below
- source_block: int32 [256, 8, 8], P('lat', 'lon'), may hold values from 0 to 7, as said below
- slot_count: int32 [256, 8], P('lat', 'lon'), may hold values from 1 to 8, as said below
Outputs:
- advected_fixed: float32 [256, 1024, 32, 4], P('lat', 'lon')
The draws below stay inside these ranges and needn't reach their ends.
Inputs may be any that keep to these rules, and one draw needn't show every extreme that they name: source_row differs from the target tile's own row by at most 4 and lies within the grid. source_block lies at cyclic distance at most 2 from the target tile's own index along the row, except for target tiles of the first and the last latitude row, where it may reach 3; the allowed distance grows from 1 at the equator towards the poles; in the two outermost rows slot 0 reaches exactly 3 sectors ahead on even tiles and 3 sectors behind on odd tiles. slot_count grows from 1 or 2 at the equator to 8 at the two outermost rows. weights are of either sign; for each target tile the weights of each target cell over the used slots and all source cells sum (before rounding to bfloat16) to one value of that tile between 0.9 and 1.05.
All inputs are finite; a program needn't handle non-finite values.
Results may differ from the reference program's by a relative error of at most 0.0003.
Values may be sent and summed in bfloat16 or wider, within the bound.
A program may use at most 192 MiB of HBM per device.

```python
import math
import jax
import jax.numpy as jnp
from jax import lax

TILE = 128
LEV = 32
TRC = 4
KMAX = 8
RLAT = 4
REACH = 3
NLAT = 256
NBLK = 8
NLON = 1024


def source_lists(key):
    base = jax.random.fold_in(key, 4711)
    first_key, second_key, third_key = jax.random.split(base, 3)
    shape = (NLAT, NBLK, KMAX)
    rows_all = jnp.arange(NLAT, dtype=jnp.int32)[:, None, None]
    distance = jnp.abs(2 * rows_all - (NLAT - 1))
    span = max((NLAT - 1) * (NLAT - 1), 1)
    extra = jax.random.randint(first_key, (NLAT, NBLK, 1), 0, 2, dtype=jnp.int32)
    counts = jnp.minimum(KMAX, 1 + (KMAX - 1) * distance * distance // span + extra)[:, :, 0]
    allowed = 1 + (REACH - 1) * distance * distance // span
    offsets = jax.random.randint(second_key, shape, -REACH, REACH + 1, dtype=jnp.int32)
    offsets = jnp.clip(offsets, -allowed, allowed)
    slots = jnp.arange(KMAX, dtype=jnp.int32)[None, None, :]
    columns = jnp.arange(NBLK, dtype=jnp.int32)[None, :, None]
    outermost = (distance == NLAT - 1) & (slots == 0)
    polar_sign = 1 - 2 * (columns % 2)
    offsets = jnp.where(outermost, allowed * polar_sign, offsets)
    blocks = (columns + offsets) % NBLK
    row_shift = jax.random.randint(third_key, shape, -RLAT, RLAT + 1, dtype=jnp.int32)
    rows_out = jnp.clip(rows_all + row_shift, 0, NLAT - 1)
    return (rows_out.astype(jnp.int32), blocks.astype(jnp.int32), counts.astype(jnp.int32))


def draw_source_row(key, part):
    return source_lists(key)[0]


def draw_source_block(key, part):
    return source_lists(key)[1]


def draw_slot_count(key, part):
    return source_lists(key)[2]


def draw_weights(key, part):
    counts = source_lists(key)[2]
    base = jax.random.fold_in(key, 911)
    spread = float(TILE * KMAX) ** (-0.5)

    def one_row(packed):
        row_number, count_row = packed
        row_key = jax.random.fold_in(base, row_number)
        noise_key, target_key = jax.random.split(row_key)
        shape = (NBLK, KMAX, TILE, TILE)
        noise = jax.random.normal(noise_key, shape, jnp.float32) * spread
        target = jax.random.uniform(target_key, (NBLK,), jnp.float32, 0.9, 1.05)
        active = (jnp.arange(KMAX, dtype=jnp.int32)[None, :] < count_row[:, None]).astype(jnp.float32)
        used = count_row.astype(jnp.float32) * TILE
        mask = active[:, :, None, None]
        row_total = jnp.sum(noise * mask, axis=(1, 3))
        offset = (target[:, None] - row_total) / used[:, None]
        result = noise + mask * offset[:, None, :, None]
        return result.astype(jnp.bfloat16)
    return lax.map(one_row, (jnp.arange(NLAT, dtype=jnp.int32), counts))


def block_scale(rng, dims, shards, smallest, top_value):
    loudness = 1.0
    for position, parts in shards:
        steps = jax.random.uniform(jax.random.fold_in(jax.random.fold_in(rng, 6), position), (parts,), jnp.float32, smallest / len(shards), top_value / len(shards))
        loudness = loudness * jnp.repeat(jnp.exp(steps), dims[position] // parts).reshape((-1,) + (1,) * (len(dims) - 1 - position))
    return loudness


def setup_inputs(seed: int = 0) -> dict:
    arg_keys = jax.random.split(jax.random.key(seed), 6)
    return {
        "tracers": jnp.clip(2.0 * jax.random.uniform(arg_keys[0], (NLAT, NLON, LEV, TRC), jnp.float32) ** block_scale(arg_keys[0], (NLAT, NLON, LEV, TRC), ((0, 4), (1, 8)), -0.2, 0.2), 0.0, 2.0).astype(jnp.bfloat16),
        "weights": draw_weights(jax.random.fold_in(arg_keys[5], 71), 0),
        "source_row": draw_source_row(jax.random.fold_in(arg_keys[5], 71), 0),
        "source_block": draw_source_block(jax.random.fold_in(arg_keys[5], 71), 0),
        "slot_count": draw_slot_count(jax.random.fold_in(arg_keys[5], 71), 0),
    }


def latitude_area(total_rows, first_row, count_rows):
    rows_all = jnp.arange(count_rows, dtype=jnp.int32) + first_row
    angle = -0.5 * math.pi + (rows_all.astype(jnp.float32) + 0.5) * (math.pi / total_rows)
    return jnp.cos(angle)


def reference(tracers, weights, source_row, source_block, slot_count):
    channels = LEV * TRC
    blocks = tracers.reshape(NLAT, NBLK, TILE, channels)

    def one_row(packed):
        rows_here, blocks_here, counts_here, weights_here = packed
        sources = blocks[rows_here, blocks_here]
        active = jnp.arange(KMAX, dtype=jnp.int32)[None, :] < counts_here[:, None]
        sources = jnp.where(active[:, :, None, None], sources, jnp.zeros((), sources.dtype))
        return jnp.einsum("bkij,bkjc->bic", weights_here.astype(jnp.float32), sources.astype(jnp.float32))

    advected = lax.map(one_row, (source_row, source_block, slot_count, weights))
    advected = advected.reshape(NLAT, NLON, channels)
    field = tracers.reshape(NLAT, NLON, channels)
    area = latitude_area(NLAT, 0, NLAT)
    total_area = NLON * jnp.sum(area)
    mass_old = jnp.sum(area[:, None, None] * field, axis=(0, 1))
    mass_new = jnp.sum(area[:, None, None] * advected, axis=(0, 1))
    fixed = advected + (mass_old - mass_new) / total_area
    return fixed.reshape(NLAT, NLON, LEV, TRC)
```

```python
import functools
import math

import jax
import jax.numpy as jnp
import numpy as np
from jax import lax
from jax.experimental import pallas as pl
from jax.experimental.pallas import tpu as pltpu
from jax.sharding import PartitionSpec as P

RLAT = 4
REACH = 3
OFFSETS = tuple(d for d in range(-REACH, REACH + 1) if d != 0)
MESH = pl.DeviceIdType.MESH
ANY = pl.BlockSpec(memory_space=pl.ANY)
VMEM = pl.BlockSpec(memory_space=pltpu.VMEM)
SMEM = pl.BlockSpec(memory_space=pltpu.SMEM)


def shifted(value, axis, by):
    length = lax.axis_size(axis)
    return lax.ppermute(value, axis, [(i, (i + by) % length) for i in range(length)])


def area_table(total_rows):
    angle = -0.5 * math.pi + (np.arange(total_rows) + 0.5) * (math.pi / total_rows)
    return np.cos(angle).astype(np.float32)


def everyone(lats, lons):
    return [(a, b) for a in range(lats) for b in range(lons) if (a, b) != (0, 0)]


def send_to_all(lats, lons, mine, slots, send_sem, recv_sem):
    lat, lon = lax.axis_index("lat"), lax.axis_index("lon")
    me = lat * lons + lon
    copies = []
    for n, (a, b) in enumerate(everyone(lats, lons)):
        peer = (lax.rem(lat + a, lats), lax.rem(lon + b, lons))
        copy = pltpu.make_async_remote_copy(
            src_ref=mine,
            dst_ref=slots.at[me],
            send_sem=send_sem.at[n],
            recv_sem=recv_sem.at[n],
            device_id=peer,
            device_id_type=MESH,
        )
        copy.start()
        copies.append(copy)
    return copies


def greet(lats, lons):
    lat, lon = lax.axis_index("lat"), lax.axis_index("lon")
    barrier = pltpu.get_barrier_semaphore()
    peers = everyone(lats, lons)
    for a, b in peers:
        peer = (lax.rem(lat + a, lats), lax.rem(lon + b, lons))
        pl.semaphore_signal(barrier, inc=1, device_id=peer, device_id_type=MESH)
    pl.semaphore_wait(barrier, len(peers))


def needs_kernel(lats, lons, need, field, slots, before, after, send_sem, recv_sem, halo_send, halo_recv):
    lat, lon = lax.axis_index("lat"), lax.axis_index("lon")
    rows = field.shape[0]
    greet(lats, lons)

    def up():
        return pltpu.make_async_remote_copy(
            src_ref=field.at[pl.ds(rows - RLAT, RLAT)],
            dst_ref=before,
            send_sem=halo_send.at[0],
            recv_sem=halo_recv.at[0],
            device_id=(lax.rem(lat + 1, lats), lon),
            device_id_type=MESH,
        )

    def down():
        return pltpu.make_async_remote_copy(
            src_ref=field.at[pl.ds(0, RLAT)],
            dst_ref=after,
            send_sem=halo_send.at[1],
            recv_sem=halo_recv.at[1],
            device_id=(lax.rem(lat + lats - 1, lats), lon),
            device_id_type=MESH,
        )

    up().start()
    down().start()
    copies = send_to_all(lats, lons, need, slots, send_sem, recv_sem)
    slots[lat * lons + lon] = need[...]
    for copy in copies:
        copy.wait()
    up().wait()
    down().wait()


def share_needs(need, field, lats, lons):
    count = lats * lons
    halo = jax.ShapeDtypeStruct((RLAT,) + field.shape[1:], field.dtype)
    return pl.pallas_call(
        functools.partial(needs_kernel, lats, lons),
        out_shape=(jax.ShapeDtypeStruct((count,) + need.shape, need.dtype), halo, halo),
        in_specs=[VMEM, ANY],
        out_specs=(VMEM, ANY, ANY),
        scratch_shapes=[
            pltpu.SemaphoreType.DMA((count - 1,)),
            pltpu.SemaphoreType.DMA((count - 1,)),
            pltpu.SemaphoreType.DMA((2,)),
            pltpu.SemaphoreType.DMA((2,)),
        ],
        compiler_params=pltpu.CompilerParams(collective_id=0, has_side_effects=True),
        name="share_needs",
    )(need, field)


def total_kernel(lats, lons, part, total, slots, send_sem, recv_sem):
    greet(lats, lons)
    copies = send_to_all(lats, lons, part, slots, send_sem, recv_sem)
    slots[lax.axis_index("lat") * lons + lax.axis_index("lon")] = part[...]
    for copy in copies:
        copy.wait()
    total[...] = jnp.sum(slots[...], axis=0)


def sum_over_devices(part, lats, lons):
    count = lats * lons
    return pl.pallas_call(
        functools.partial(total_kernel, lats, lons),
        out_shape=jax.ShapeDtypeStruct(part.shape, part.dtype),
        in_specs=[VMEM],
        out_specs=VMEM,
        scratch_shapes=[
            pltpu.VMEM((count,) + part.shape, part.dtype),
            pltpu.SemaphoreType.DMA((count - 1,)),
            pltpu.SemaphoreType.DMA((count - 1,)),
        ],
        compiler_params=pltpu.CompilerParams(collective_id=1, has_side_effects=True),
        name="sum_masses",
    )(part)


def capacities(padded_rows):
    caps = {}
    for d in OFFSETS:
        if abs(d) == 1:
            caps[d] = (padded_rows * 7 // 9, padded_rows * 2 // 3)
        elif abs(d) == 2:
            caps[d] = (padded_rows * 7 // 12, 0)
        else:
            caps[d] = (RLAT + 1, 0)
    return caps


def exchange_kernel(
    lats, lons, caps, bases, lists, field, before, after, recv, padded, outgoing, load_sem, send_sem, recv_sem
):
    lat, lon = lax.axis_index("lat"), lax.axis_index("lon")
    rows = field.shape[0]
    loads = [
        pltpu.make_async_copy(before, padded.at[pl.ds(0, RLAT)], load_sem.at[0]),
        pltpu.make_async_copy(field, padded.at[pl.ds(RLAT, rows)], load_sem.at[1]),
        pltpu.make_async_copy(after, padded.at[pl.ds(RLAT + rows, RLAT)], load_sem.at[2]),
    ]
    for load in loads:
        load.start()
    barrier = pltpu.get_barrier_semaphore()
    for d in OFFSETS:
        peer = (lat, lax.rem(lon + lons - d, lons))
        pl.semaphore_signal(barrier, inc=1, device_id=peer, device_id_type=MESH)
    pl.semaphore_wait(barrier, len(OFFSETS))
    for load in loads:
        load.wait()

    polar = (lat == 0) | (lat == lats - 1)
    pieces = []
    for d in sorted(OFFSETS, key=lambda d: (abs(d), d)):
        outer, inner = caps[d]
        if inner:
            pieces.append((d, 0, inner, False))
    for d in sorted(OFFSETS, key=lambda d: (abs(d) == 1, abs(d), d)):
        outer, inner = caps[d]
        if outer > inner:
            pieces.append((d, inner, outer, True))

    def guarded(only_polar, act):
        if only_polar:
            pl.when(polar)(act)
        else:
            act()

    def copy_of(n):
        d, first, last, _ = pieces[n]
        span = pl.ds(bases[d] + first, last - first)
        return pltpu.make_async_remote_copy(
            src_ref=outgoing.at[span],
            dst_ref=recv.at[span],
            send_sem=send_sem.at[n],
            recv_sem=recv_sem.at[n],
            device_id=(lat, lax.rem(lon + lons - d, lons)),
            device_id_type=MESH,
        )

    def gather(n):
        d, first, last, _ = pieces[n]
        row = OFFSETS.index(d)

        def step(c, carry):
            outgoing[bases[d] + c] = padded[lists[row, c]]
            return carry

        lax.fori_loop(first, last, step, 0)

    for n in range(len(pieces) + 1):
        if n < len(pieces):
            guarded(pieces[n][3], functools.partial(gather, n))
        if n > 0:
            guarded(pieces[n - 1][3], lambda n=n: copy_of(n - 1).start())
    for n in range(len(pieces)):
        guarded(pieces[n][3], lambda n=n: copy_of(n).wait())


def exchange(lists, field, before, after, lats, lons, caps, bases, received):
    tile = field.shape[1:]
    padded_rows = field.shape[0] + 2 * RLAT
    count = 2 * len(OFFSETS)
    return pl.pallas_call(
        functools.partial(exchange_kernel, lats, lons, caps, bases),
        out_shape=jax.ShapeDtypeStruct((received,) + tile, field.dtype),
        in_specs=[SMEM, ANY, ANY, ANY],
        out_specs=ANY,
        scratch_shapes=[
            pltpu.VMEM((padded_rows,) + tile, field.dtype),
            pltpu.VMEM((received,) + tile, field.dtype),
            pltpu.SemaphoreType.DMA((3,)),
            pltpu.SemaphoreType.DMA((count,)),
            pltpu.SemaphoreType.DMA((count,)),
        ],
        compiler_params=pltpu.CompilerParams(collective_id=2, has_side_effects=True),
        name="exchange",
    )(lists, field, before, after)


def advect_kernel(step_rows, slots, index, counts, area, weights, field, before, after, recv, out, delta, src, gap, sem):
    g = pl.program_id(0)
    rows = field.shape[0]
    padded_rows = rows + 2 * RLAT
    received = recv.shape[0]

    @pl.when(g == 0)
    def _():
        loads = [
            pltpu.make_async_copy(before, src.at[pl.ds(0, RLAT)], sem.at[0]),
            pltpu.make_async_copy(field, src.at[pl.ds(RLAT, rows)], sem.at[1]),
            pltpu.make_async_copy(after, src.at[pl.ds(RLAT + rows, RLAT)], sem.at[2]),
            pltpu.make_async_copy(recv, src.at[pl.ds(padded_rows, received)], sem.at[3]),
        ]
        for load in loads:
            load.start()
        src[padded_rows + received] = jnp.zeros(src.shape[1:], src.dtype)
        gap[...] = jnp.zeros_like(gap)
        for load in loads:
            load.wait()

    for tt in range(step_rows):
        t = g * step_rows + tt
        used = counts[t]
        for last in range(2, slots + 2, 2):
            width = min(last, slots)

            @pl.when((used > last - 2) & (used <= last))
            def _(tt=tt, t=t, width=width):
                left = jnp.concatenate([src[index[t * slots + k]] for k in range(width)], axis=1)
                right = jnp.concatenate([weights[tt, 0, k] for k in range(width)], axis=1)
                out[tt] = lax.dot_general(
                    left, right, (((1,), (1,)), ((), ())), preferred_element_type=jnp.float32
                )

        gap[...] += area[t] * (src[RLAT + t].astype(jnp.float32) - out[tt])

    @pl.when(g == pl.num_programs(0) - 1)
    def _():
        sums = jnp.sum(gap[...].T, axis=0, keepdims=True)
        delta[...] = jnp.broadcast_to(sums, delta.shape)


def advect(index, counts, area, weights, field, before, after, recv):
    rows, channels, width = field.shape
    slots = weights.shape[2]
    step_rows = 4
    while rows % step_rows:
        step_rows -= 1
    sources = rows + 2 * RLAT + recv.shape[0] + 1
    block = (step_rows,) + weights.shape[1:]
    return pl.pallas_call(
        functools.partial(advect_kernel, step_rows, slots),
        grid=(rows // step_rows,),
        out_shape=(
            jax.ShapeDtypeStruct(field.shape, jnp.float32),
            jax.ShapeDtypeStruct((8, channels), jnp.float32),
        ),
        in_specs=[
            SMEM,
            SMEM,
            SMEM,
            pl.BlockSpec(block, lambda g: (g, 0, 0, 0, 0)),
            ANY,
            ANY,
            ANY,
            ANY,
        ],
        out_specs=(
            pl.BlockSpec((step_rows, channels, width), lambda g: (g, 0, 0)),
            pl.BlockSpec((8, channels), lambda g: (0, 0)),
        ),
        scratch_shapes=[
            pltpu.VMEM((sources, channels, width), field.dtype),
            pltpu.VMEM((channels, width), jnp.float32),
            pltpu.SemaphoreType.DMA((4,)),
        ],
        compiler_params=pltpu.CompilerParams(dimension_semantics=("arbitrary",)),
        name="advect",
    )(index, counts, area, weights, field, before, after, recv)


def dense(field, before, after, weights, local_row, relative, active, area):
    padded = jnp.concatenate([before, field, after], axis=0)
    stack = jnp.stack(
        [padded if d == 0 else shifted(padded, "lon", -d) for d in range(-REACH, REACH + 1)], axis=1
    )
    rows = jnp.clip(local_row, 0, padded.shape[0] - 1)
    picked = stack[rows, jnp.clip(relative + REACH, 0, 2 * REACH)]
    picked = jnp.where(active[:, :, None, None], picked, jnp.zeros((), picked.dtype))
    advected = jnp.einsum("tkij,tkcj->tci", weights[:, 0], picked, preferred_element_type=jnp.float32)
    gap = jnp.sum(area[:, None, None] * (field.astype(jnp.float32) - advected), axis=(0, 2))
    return advected, jnp.broadcast_to(gap[None, :], (8, gap.shape[0]))


def local(tracers, weights, source_row, source_block, slot_count):
    rows, width, levels, kinds = tracers.shape
    channels = levels * kinds
    lats, lons = lax.axis_size("lat"), lax.axis_size("lon")
    lat, lon = lax.axis_index("lat"), lax.axis_index("lon")
    field = tracers.reshape(rows, width, channels).transpose(0, 2, 1)
    slots = source_row.shape[2]
    table = area_table(rows * lats)
    total_area = float(width * lons * np.sum(table.astype(np.float64)))
    area = lax.dynamic_slice(jnp.asarray(table), (lat * rows,), (rows,))

    padded_rows = rows + 2 * RLAT
    lanes = -(-padded_rows // 128) * 128
    local_row = source_row[:, 0, :] - (lat * rows - RLAT)
    relative = (source_block[:, 0, :] - lon + REACH) % lons - REACH
    active = jnp.arange(slots, dtype=jnp.int32)[None, :] < slot_count
    remote = active & (relative != 0)
    which = jnp.where(relative < 0, relative + REACH, relative + REACH - 1)
    code = jnp.where(remote, which * lanes + local_row, -1).reshape(-1)
    hit = code[None, :] == jnp.arange(8 * lanes, dtype=jnp.int32)[:, None]
    need = jnp.any(hit, axis=1).astype(jnp.float32).reshape(8, lanes)

    needs, before, after = share_needs(need, field, lats, lons)

    caps = capacities(padded_rows)
    bases, received = {}, 0
    for d in OFFSETS:
        bases[d] = received
        received += max(caps[d])
    limit = np.zeros((lats, lons, 8), np.float32)
    for n, d in enumerate(OFFSETS):
        limit[:, :, n] = caps[d][1]
        limit[0, :, n] = limit[-1, :, n] = caps[d][0]
    over = jnp.any(jnp.sum(needs, axis=2) > jnp.asarray(limit.reshape(lats * lons, 8)))

    upto = (jnp.arange(lanes)[:, None] <= jnp.arange(lanes)[None, :]).astype(jnp.float32)

    def ranks(mask):
        return jnp.sum(mask[:, :, None] * upto[None], axis=1).astype(jnp.int32) - 1

    def fast(field, before, after, weights, needs):
        band = lax.dynamic_slice(needs, (lat * lons, 0, 0), (lons, 8, lanes))
        offsets = np.zeros((8,), np.int32)
        offsets[: len(OFFSETS)] = OFFSETS
        dest = (lon - jnp.asarray(offsets)) % lons
        chosen = jnp.arange(lons, dtype=jnp.int32)[:, None] == dest[None, :]
        wanted = jnp.sum(jnp.where(chosen[:, :, None], band, 0.0), axis=0)
        rank = jnp.where(wanted > 0, ranks(wanted), -1)
        place = jnp.arange(lanes, dtype=jnp.int32)
        match = rank[:, :, None] == place[None, None, :]
        lists = jnp.sum(jnp.where(match, place[None, :, None], 0), axis=1)
        recv = exchange(lists, field, before, after, lats, lons, caps, bases, received)
        start = np.zeros((8,), np.int32)
        start[: len(OFFSETS)] = [bases[d] + padded_rows for d in OFFSETS]
        where = (ranks(need) + jnp.asarray(start)[:, None]).reshape(-1)
        index = jnp.sum(jnp.where(hit, where[:, None], 0), axis=0)
        own = jnp.where(active, local_row, padded_rows + received).reshape(-1)
        index = jnp.where(remote.reshape(-1), index, own)
        return advect(index, slot_count[:, 0], area, weights, field, before, after, recv)

    def general(field, before, after, weights, needs):
        return dense(field, before, after, weights, local_row, relative, active, area)

    advected, delta = lax.cond(over, general, fast, field, before, after, weights, needs)
    total = sum_over_devices(delta, lats, lons)
    fixed = advected + (total[0] / total_area)[None, :, None]
    return fixed.transpose(0, 2, 1).reshape(rows, width, levels, kinds)


def solution(mesh):
    return jax.shard_map(
        local,
        mesh=mesh,
        in_specs=(
            P("lat", "lon", None, None),
            P("lat", "lon", None, None, None),
            P("lat", "lon", None),
            P("lat", "lon", None),
            P("lat", "lon"),
        ),
        out_specs=P("lat", "lon", None, None),
        check_vma=False,
    )
```

```python
import functools
import math

import jax
import jax.numpy as jnp
import numpy as np
from jax import lax
from jax.experimental import pallas as pl
from jax.experimental.pallas import tpu as pltpu
from jax.sharding import PartitionSpec as P

RLAT = 4
REACH = 3
OFFSETS = tuple(d for d in range(-REACH, REACH + 1) if d != 0)
MESH = pl.DeviceIdType.MESH
ANY = pl.BlockSpec(memory_space=pl.ANY)
VMEM = pl.BlockSpec(memory_space=pltpu.VMEM)
SMEM = pl.BlockSpec(memory_space=pltpu.SMEM)


def shifted(value, axis, by):
    length = lax.axis_size(axis)
    return lax.ppermute(value, axis, [(i, (i + by) % length) for i in range(length)])


def area_table(total_rows):
    angle = -0.5 * math.pi + (np.arange(total_rows) + 0.5) * (math.pi / total_rows)
    return np.cos(angle).astype(np.float32)


def everyone(lats, lons):
    return [(a, b) for a in range(lats) for b in range(lons) if (a, b) != (0, 0)]


def send_to_all(lats, lons, mine, slots, send_sem, recv_sem):
    lat, lon = lax.axis_index("lat"), lax.axis_index("lon")
    me = lat * lons + lon
    copies = []
    for n, (a, b) in enumerate(everyone(lats, lons)):
        peer = (lax.rem(lat + a, lats), lax.rem(lon + b, lons))
        copy = pltpu.make_async_remote_copy(
            src_ref=mine,
            dst_ref=slots.at[me],
            send_sem=send_sem.at[n],
            recv_sem=recv_sem.at[n],
            device_id=peer,
            device_id_type=MESH,
        )
        copy.start()
        copies.append(copy)
    return copies


def greet(lats, lons):
    lat, lon = lax.axis_index("lat"), lax.axis_index("lon")
    barrier = pltpu.get_barrier_semaphore()
    peers = everyone(lats, lons)
    for a, b in peers:
        peer = (lax.rem(lat + a, lats), lax.rem(lon + b, lons))
        pl.semaphore_signal(barrier, inc=1, device_id=peer, device_id_type=MESH)
    pl.semaphore_wait(barrier, len(peers))


def needs_kernel(lats, lons, need, field, slots, before, after, send_sem, recv_sem, halo_send, halo_recv):
    lat, lon = lax.axis_index("lat"), lax.axis_index("lon")
    rows = field.shape[0]
    greet(lats, lons)

    def up():
        return pltpu.make_async_remote_copy(
            src_ref=field.at[pl.ds(rows - RLAT, RLAT)],
            dst_ref=before,
            send_sem=halo_send.at[0],
            recv_sem=halo_recv.at[0],
            device_id=(lax.rem(lat + 1, lats), lon),
            device_id_type=MESH,
        )

    def down():
        return pltpu.make_async_remote_copy(
            src_ref=field.at[pl.ds(0, RLAT)],
            dst_ref=after,
            send_sem=halo_send.at[1],
            recv_sem=halo_recv.at[1],
            device_id=(lax.rem(lat + lats - 1, lats), lon),
            device_id_type=MESH,
        )

    up().start()
    down().start()
    copies = send_to_all(lats, lons, need, slots, send_sem, recv_sem)
    slots[lat * lons + lon] = need[...]
    for copy in copies:
        copy.wait()
    up().wait()
    down().wait()


def share_needs(need, field, lats, lons):
    count = lats * lons
    halo = jax.ShapeDtypeStruct((RLAT,) + field.shape[1:], field.dtype)
    return pl.pallas_call(
        functools.partial(needs_kernel, lats, lons),
        out_shape=(jax.ShapeDtypeStruct((count,) + need.shape, need.dtype), halo, halo),
        in_specs=[VMEM, ANY],
        out_specs=(VMEM, ANY, ANY),
        scratch_shapes=[
            pltpu.SemaphoreType.DMA((count - 1,)),
            pltpu.SemaphoreType.DMA((count - 1,)),
            pltpu.SemaphoreType.DMA((2,)),
            pltpu.SemaphoreType.DMA((2,)),
        ],
        compiler_params=pltpu.CompilerParams(collective_id=0, has_side_effects=True),
        name="share_needs",
    )(need, field)


def total_kernel(lats, lons, part, total, slots, send_sem, recv_sem):
    greet(lats, lons)
    copies = send_to_all(lats, lons, part, slots, send_sem, recv_sem)
    slots[lax.axis_index("lat") * lons + lax.axis_index("lon")] = part[...]
    for copy in copies:
        copy.wait()
    total[...] = jnp.sum(slots[...], axis=0)


def sum_over_devices(part, lats, lons):
    count = lats * lons
    return pl.pallas_call(
        functools.partial(total_kernel, lats, lons),
        out_shape=jax.ShapeDtypeStruct(part.shape, part.dtype),
        in_specs=[VMEM],
        out_specs=VMEM,
        scratch_shapes=[
            pltpu.VMEM((count,) + part.shape, part.dtype),
            pltpu.SemaphoreType.DMA((count - 1,)),
            pltpu.SemaphoreType.DMA((count - 1,)),
        ],
        compiler_params=pltpu.CompilerParams(collective_id=1, has_side_effects=True),
        name="sum_masses",
    )(part)


TIERS = ((52, 44, 39), (60, 52, 46))


def capacities(padded_rows, tier):
    near_polar, near_inner, far_polar = [padded_rows * part // 72 for part in tier]
    by_reach = {1: (near_polar, near_inner), 2: (far_polar, 0)}
    return {d: by_reach.get(abs(d), (RLAT + 1, 0)) for d in OFFSETS}


def layout_of(caps):
    bases, received = {}, 0
    for d in OFFSETS:
        bases[d] = received
        received += max(caps[d])
    return bases, received


def exchange_kernel(
    lats, lons, caps, bases, lists, field, before, after, recv, padded, outgoing, load_sem, send_sem, recv_sem
):
    lat, lon = lax.axis_index("lat"), lax.axis_index("lon")
    rows = field.shape[0]
    loads = [
        pltpu.make_async_copy(before, padded.at[pl.ds(0, RLAT)], load_sem.at[0]),
        pltpu.make_async_copy(field, padded.at[pl.ds(RLAT, rows)], load_sem.at[1]),
        pltpu.make_async_copy(after, padded.at[pl.ds(RLAT + rows, RLAT)], load_sem.at[2]),
    ]
    for load in loads:
        load.start()
    barrier = pltpu.get_barrier_semaphore()
    for d in OFFSETS:
        peer = (lat, lax.rem(lon + lons - d, lons))
        pl.semaphore_signal(barrier, inc=1, device_id=peer, device_id_type=MESH)
    pl.semaphore_wait(barrier, len(OFFSETS))
    for load in loads:
        load.wait()

    polar = (lat == 0) | (lat == lats - 1)
    pieces = []
    for d in sorted(OFFSETS, key=lambda d: (abs(d), d)):
        outer, inner = caps[d]
        if inner:
            pieces.append((d, 0, inner, False))
    for d in sorted(OFFSETS, key=lambda d: (abs(d) == 1, abs(d), d)):
        outer, inner = caps[d]
        if outer > inner:
            pieces.append((d, inner, outer, True))

    def guarded(only_polar, act):
        if only_polar:
            pl.when(polar)(act)
        else:
            act()

    def copy_of(n):
        d, first, last, _ = pieces[n]
        span = pl.ds(bases[d] + first, last - first)
        return pltpu.make_async_remote_copy(
            src_ref=outgoing.at[span],
            dst_ref=recv.at[span],
            send_sem=send_sem.at[n],
            recv_sem=recv_sem.at[n],
            device_id=(lat, lax.rem(lon + lons - d, lons)),
            device_id_type=MESH,
        )

    def gather(n):
        d, first, last, _ = pieces[n]
        row = OFFSETS.index(d)

        def step(c, carry):
            outgoing[bases[d] + c] = padded[lists[row, c]]
            return carry

        lax.fori_loop(first, last, step, 0)

    for n in range(len(pieces) + 1):
        if n < len(pieces):
            guarded(pieces[n][3], functools.partial(gather, n))
        if n > 0:
            guarded(pieces[n - 1][3], lambda n=n: copy_of(n - 1).start())
    for n in range(len(pieces)):
        guarded(pieces[n][3], lambda n=n: copy_of(n).wait())


def exchange(lists, field, before, after, lats, lons, caps, bases, received, collective_id):
    tile = field.shape[1:]
    padded_rows = field.shape[0] + 2 * RLAT
    count = 2 * len(OFFSETS)
    return pl.pallas_call(
        functools.partial(exchange_kernel, lats, lons, caps, bases),
        out_shape=jax.ShapeDtypeStruct((received,) + tile, field.dtype),
        in_specs=[SMEM, ANY, ANY, ANY],
        out_specs=ANY,
        scratch_shapes=[
            pltpu.VMEM((padded_rows,) + tile, field.dtype),
            pltpu.VMEM((received,) + tile, field.dtype),
            pltpu.SemaphoreType.DMA((3,)),
            pltpu.SemaphoreType.DMA((count,)),
            pltpu.SemaphoreType.DMA((count,)),
        ],
        compiler_params=pltpu.CompilerParams(collective_id=collective_id, has_side_effects=True),
        name="exchange",
    )(lists, field, before, after)


def advect_kernel(step_rows, slots, index, counts, area, weights, field, before, after, recv, out, delta, src, gap, sem):
    g = pl.program_id(0)
    rows = field.shape[0]
    padded_rows = rows + 2 * RLAT
    received = recv.shape[0]

    @pl.when(g == 0)
    def _():
        loads = [
            pltpu.make_async_copy(before, src.at[pl.ds(0, RLAT)], sem.at[0]),
            pltpu.make_async_copy(field, src.at[pl.ds(RLAT, rows)], sem.at[1]),
            pltpu.make_async_copy(after, src.at[pl.ds(RLAT + rows, RLAT)], sem.at[2]),
            pltpu.make_async_copy(recv, src.at[pl.ds(padded_rows, received)], sem.at[3]),
        ]
        for load in loads:
            load.start()
        src[padded_rows + received] = jnp.zeros(src.shape[1:], src.dtype)
        gap[...] = jnp.zeros_like(gap)
        for load in loads:
            load.wait()

    used = counts[g * step_rows]
    for tt in range(1, step_rows):
        used = jnp.maximum(used, counts[g * step_rows + tt])
    for last in range(2, slots + 2, 2):
        width = min(last, slots)

        @pl.when((used > last - 2) & (used <= last))
        def _(width=width):
            total = gap[...]
            for tt in range(step_rows):
                t = g * step_rows + tt
                left = jnp.concatenate([src[index[k, t]] for k in range(width)], axis=1)
                right = jnp.concatenate([weights[tt, 0, k] for k in range(width)], axis=1)
                value = lax.dot_general(
                    left, right, (((1,), (1,)), ((), ())), preferred_element_type=jnp.float32
                )
                out[tt] = value
                total += area[t] * (src[RLAT + t].astype(jnp.float32) - value)
            gap[...] = total

    @pl.when(g == pl.num_programs(0) - 1)
    def _():
        delta[...] = jnp.sum(gap[...].T, axis=0, keepdims=True)


def advect(index, counts, area, weights, field, before, after, recv):
    rows, channels, width = field.shape
    slots = weights.shape[2]
    step_rows = 4
    while rows % step_rows:
        step_rows -= 1
    sources = rows + 2 * RLAT + recv.shape[0] + 1
    block = (step_rows,) + weights.shape[1:]
    return pl.pallas_call(
        functools.partial(advect_kernel, step_rows, slots),
        grid=(rows // step_rows,),
        out_shape=(
            jax.ShapeDtypeStruct(field.shape, jnp.float32),
            jax.ShapeDtypeStruct((1, channels), jnp.float32),
        ),
        in_specs=[
            SMEM,
            SMEM,
            SMEM,
            pl.BlockSpec(block, lambda g: (g, 0, 0, 0, 0)),
            ANY,
            ANY,
            ANY,
            ANY,
        ],
        out_specs=(
            pl.BlockSpec((step_rows, channels, width), lambda g: (g, 0, 0)),
            pl.BlockSpec((1, channels), lambda g: (0, 0)),
        ),
        scratch_shapes=[
            pltpu.VMEM((sources, channels, width), field.dtype),
            pltpu.VMEM((channels, width), jnp.float32),
            pltpu.SemaphoreType.DMA((4,)),
        ],
        compiler_params=pltpu.CompilerParams(dimension_semantics=("arbitrary",)),
        name="advect",
    )(index, counts, area, weights, field, before, after, recv)


def dense(field, before, after, weights, local_row, relative, active, area):
    padded = jnp.concatenate([before, field, after], axis=0)
    stack = jnp.stack(
        [padded if d == 0 else shifted(padded, "lon", -d) for d in range(-REACH, REACH + 1)], axis=1
    )
    rows = jnp.clip(local_row, 0, padded.shape[0] - 1)
    picked = stack[rows, jnp.clip(relative + REACH, 0, 2 * REACH)]
    picked = jnp.where(active[:, :, None, None], picked, jnp.zeros((), picked.dtype))
    advected = jnp.einsum("tkij,ktcj->tci", weights[:, 0], picked, preferred_element_type=jnp.float32)
    gap = jnp.sum(area[:, None, None] * (field.astype(jnp.float32) - advected), axis=(0, 2))
    return advected, gap[None, :]


def local(tracers, weights, source_row, source_block, slot_count):
    rows, width, levels, kinds = tracers.shape
    channels = levels * kinds
    lats, lons = lax.axis_size("lat"), lax.axis_size("lon")
    lat, lon = lax.axis_index("lat"), lax.axis_index("lon")
    field = tracers.reshape(rows, width, channels).transpose(0, 2, 1)
    slots = source_row.shape[2]
    table = area_table(rows * lats)
    total_area = float(width * lons * np.sum(table.astype(np.float64)))
    area = lax.dynamic_slice(jnp.asarray(table), (lat * rows,), (rows,))

    padded_rows = rows + 2 * RLAT
    lanes = -(-padded_rows // 128) * 128
    local_row = source_row[:, 0, :].T - (lat * rows - RLAT)
    relative = (source_block[:, 0, :].T - lon + REACH) % lons - REACH
    active = jnp.arange(slots, dtype=jnp.int32)[:, None] < slot_count[:, 0][None, :]
    remote = active & (relative != 0)
    which = jnp.where(relative < 0, relative + REACH, relative + REACH - 1)
    code = jnp.where(remote, which * lanes + local_row, -1)
    ids = jnp.arange(8 * lanes, dtype=jnp.int32).reshape(8, lanes)
    hit = code[None, None, :, :] == ids[:, :, None, None]
    need = jnp.any(hit, axis=(2, 3)).astype(jnp.bfloat16)

    needs, before, after = share_needs(need, field, lats, lons)

    plans = [capacities(padded_rows, tier) for tier in TIERS]
    counted = jnp.sum(needs.astype(jnp.float32), axis=2)
    level = jnp.int32(0)
    for caps in plans:
        limit = np.zeros((lats, lons, 8), np.float32)
        for n, d in enumerate(OFFSETS):
            limit[:, :, n] = caps[d][1]
            limit[0, :, n] = limit[-1, :, n] = caps[d][0]
        over = jnp.any(counted > jnp.asarray(limit.reshape(lats * lons, 8)))
        level += over.astype(jnp.int32)

    upto = (jnp.arange(lanes)[:, None] <= jnp.arange(lanes)[None, :]).astype(jnp.float32)

    def ranks(mask):
        mask = mask.astype(jnp.float32)
        return jnp.sum(mask[:, :, None] * upto[None], axis=1).astype(jnp.int32) - 1

    def fast(n, field, before, after, weights, needs):
        caps = plans[n]
        bases, received = layout_of(caps)
        band = lax.dynamic_slice(needs, (lat * lons, 0, 0), (lons, 8, lanes))
        offsets = np.zeros((8,), np.int32)
        offsets[: len(OFFSETS)] = OFFSETS
        dest = (lon - jnp.asarray(offsets)) % lons
        chosen = jnp.arange(lons, dtype=jnp.int32)[:, None] == dest[None, :]
        wanted = jnp.sum(jnp.where(chosen[:, :, None], band.astype(jnp.float32), 0.0), axis=0)
        rank = jnp.where(wanted > 0, ranks(wanted), -1)
        place = jnp.arange(lanes, dtype=jnp.int32)
        match = rank[:, :, None] == place[None, None, :]
        lists = jnp.sum(jnp.where(match, place[None, :, None], 0), axis=1)
        recv = exchange(lists, field, before, after, lats, lons, caps, bases, received, 2 + n)
        start = np.zeros((8,), np.int32)
        start[: len(OFFSETS)] = [bases[d] + padded_rows for d in OFFSETS]
        where = ranks(need) + jnp.asarray(start)[:, None]
        index = jnp.sum(jnp.where(hit, where[:, :, None, None], 0), axis=(0, 1))
        own = jnp.where(active, local_row, padded_rows + received)
        index = jnp.where(remote, index, own)
        return advect(index, slot_count[:, 0], area, weights, field, before, after, recv)

    def general(field, before, after, weights, needs):
        return dense(field, before, after, weights, local_row, relative, active, area)

    paths = [functools.partial(fast, n) for n in range(len(plans))] + [general]
    advected, delta = lax.switch(level, paths, field, before, after, weights, needs)
    total = sum_over_devices(delta, lats, lons)
    fixed = advected + (total[0] / total_area)[None, :, None]
    return fixed.transpose(0, 2, 1).reshape(rows, width, levels, kinds)


def solution(mesh):
    return jax.shard_map(
        local,
        mesh=mesh,
        in_specs=(
            P("lat", "lon", None, None),
            P("lat", "lon", None, None, None),
            P("lat", "lon", None),
            P("lat", "lon", None),
            P("lat", "lon"),
        ),
        out_specs=P("lat", "lon", None, None),
        check_vma=False,
    )
```

```python
import functools
import math

import jax
import jax.numpy as jnp
import numpy as np
from jax import lax
from jax.experimental import pallas as pl
from jax.experimental.pallas import tpu as pltpu
from jax.sharding import PartitionSpec as P

RLAT = 4
REACH = 3
OFFSETS = tuple(d for d in range(-REACH, REACH + 1) if d != 0)
MESH = pl.DeviceIdType.MESH
ANY = pl.BlockSpec(memory_space=pl.ANY)
VMEM = pl.BlockSpec(memory_space=pltpu.VMEM)
SMEM = pl.BlockSpec(memory_space=pltpu.SMEM)


def shifted(value, axis, by):
    length = lax.axis_size(axis)
    return lax.ppermute(value, axis, [(i, (i + by) % length) for i in range(length)])


def area_table(total_rows):
    angle = -0.5 * math.pi + (np.arange(total_rows) + 0.5) * (math.pi / total_rows)
    return np.cos(angle).astype(np.float32)


def everyone(lats, lons):
    return [(a, b) for a in range(lats) for b in range(lons) if (a, b) != (0, 0)]


def send_to_all(lats, lons, mine, slots, send_sem, recv_sem):
    lat, lon = lax.axis_index("lat"), lax.axis_index("lon")
    me = lat * lons + lon
    copies = []
    for n, (a, b) in enumerate(everyone(lats, lons)):
        peer = (lax.rem(lat + a, lats), lax.rem(lon + b, lons))
        copy = pltpu.make_async_remote_copy(
            src_ref=mine,
            dst_ref=slots.at[me],
            send_sem=send_sem.at[n],
            recv_sem=recv_sem.at[n],
            device_id=peer,
            device_id_type=MESH,
        )
        copy.start()
        copies.append(copy)
    return copies


def greet(lats, lons):
    lat, lon = lax.axis_index("lat"), lax.axis_index("lon")
    barrier = pltpu.get_barrier_semaphore()
    peers = everyone(lats, lons)
    for a, b in peers:
        peer = (lax.rem(lat + a, lats), lax.rem(lon + b, lons))
        pl.semaphore_signal(barrier, inc=1, device_id=peer, device_id_type=MESH)
    pl.semaphore_wait(barrier, len(peers))


def needs_kernel(lats, lons, need, field, slots, before, after, send_sem, recv_sem, halo_send, halo_recv):
    lat, lon = lax.axis_index("lat"), lax.axis_index("lon")
    rows = field.shape[0]
    greet(lats, lons)

    def up():
        return pltpu.make_async_remote_copy(
            src_ref=field.at[pl.ds(rows - RLAT, RLAT)],
            dst_ref=before,
            send_sem=halo_send.at[0],
            recv_sem=halo_recv.at[0],
            device_id=(lax.rem(lat + 1, lats), lon),
            device_id_type=MESH,
        )

    def down():
        return pltpu.make_async_remote_copy(
            src_ref=field.at[pl.ds(0, RLAT)],
            dst_ref=after,
            send_sem=halo_send.at[1],
            recv_sem=halo_recv.at[1],
            device_id=(lax.rem(lat + lats - 1, lats), lon),
            device_id_type=MESH,
        )

    up().start()
    down().start()
    copies = send_to_all(lats, lons, need, slots, send_sem, recv_sem)
    slots[lat * lons + lon] = need[...]
    for copy in copies:
        copy.wait()
    up().wait()
    down().wait()


def share_needs(need, field, lats, lons):
    count = lats * lons
    halo = jax.ShapeDtypeStruct((RLAT,) + field.shape[1:], field.dtype)
    return pl.pallas_call(
        functools.partial(needs_kernel, lats, lons),
        out_shape=(jax.ShapeDtypeStruct((count,) + need.shape, need.dtype), halo, halo),
        in_specs=[VMEM, ANY],
        out_specs=(VMEM, ANY, ANY),
        scratch_shapes=[
            pltpu.SemaphoreType.DMA((count - 1,)),
            pltpu.SemaphoreType.DMA((count - 1,)),
            pltpu.SemaphoreType.DMA((2,)),
            pltpu.SemaphoreType.DMA((2,)),
        ],
        compiler_params=pltpu.CompilerParams(collective_id=0, has_side_effects=True),
        name="share_needs",
    )(need, field)


def total_kernel(lats, lons, part, total, slots, send_sem, recv_sem):
    greet(lats, lons)
    copies = send_to_all(lats, lons, part, slots, send_sem, recv_sem)
    slots[lax.axis_index("lat") * lons + lax.axis_index("lon")] = part[...]
    for copy in copies:
        copy.wait()
    total[...] = jnp.sum(slots[...], axis=0)


def sum_over_devices(part, lats, lons):
    count = lats * lons
    return pl.pallas_call(
        functools.partial(total_kernel, lats, lons),
        out_shape=jax.ShapeDtypeStruct(part.shape, part.dtype),
        in_specs=[VMEM],
        out_specs=VMEM,
        scratch_shapes=[
            pltpu.VMEM((count,) + part.shape, part.dtype),
            pltpu.SemaphoreType.DMA((count - 1,)),
            pltpu.SemaphoreType.DMA((count - 1,)),
        ],
        compiler_params=pltpu.CompilerParams(collective_id=1, has_side_effects=True),
        name="sum_masses",
    )(part)


TIERS = ((52, 44, 39), (60, 52, 46))


def capacities(padded_rows, tier):
    near_polar, near_inner, far_polar = [padded_rows * part // 72 for part in tier]
    by_reach = {1: (near_polar, near_inner), 2: (far_polar, 0)}
    return {d: by_reach.get(abs(d), (RLAT + 1, 0)) for d in OFFSETS}


def layout_of(caps):
    bases, received = {}, 0
    for d in OFFSETS:
        bases[d] = received
        received += max(caps[d])
    return bases, received


def exchange_kernel(
    lats, lons, caps, bases, lists, field, before, after, recv, padded, outgoing, load_sem, send_sem, recv_sem
):
    lat, lon = lax.axis_index("lat"), lax.axis_index("lon")
    rows = field.shape[0]
    loads = [
        pltpu.make_async_copy(before, padded.at[pl.ds(0, RLAT)], load_sem.at[0]),
        pltpu.make_async_copy(field, padded.at[pl.ds(RLAT, rows)], load_sem.at[1]),
        pltpu.make_async_copy(after, padded.at[pl.ds(RLAT + rows, RLAT)], load_sem.at[2]),
    ]
    for load in loads:
        load.start()
    barrier = pltpu.get_barrier_semaphore()
    for d in OFFSETS:
        peer = (lat, lax.rem(lon + lons - d, lons))
        pl.semaphore_signal(barrier, inc=1, device_id=peer, device_id_type=MESH)
    pl.semaphore_wait(barrier, len(OFFSETS))
    for load in loads:
        load.wait()

    polar = (lat == 0) | (lat == lats - 1)
    pieces = []
    for d in sorted(OFFSETS, key=lambda d: (abs(d), d)):
        outer, inner = caps[d]
        if inner:
            pieces.append((d, 0, inner, False))
    for d in sorted(OFFSETS, key=lambda d: (abs(d) == 1, abs(d), d)):
        outer, inner = caps[d]
        if outer > inner:
            pieces.append((d, inner, outer, True))

    def guarded(only_polar, act):
        if only_polar:
            pl.when(polar)(act)
        else:
            act()

    def copy_of(n):
        d, first, last, _ = pieces[n]
        span = pl.ds(bases[d] + first, last - first)
        return pltpu.make_async_remote_copy(
            src_ref=outgoing.at[span],
            dst_ref=recv.at[span],
            send_sem=send_sem.at[n],
            recv_sem=recv_sem.at[n],
            device_id=(lat, lax.rem(lon + lons - d, lons)),
            device_id_type=MESH,
        )

    def gather(n):
        d, first, last, _ = pieces[n]
        row = OFFSETS.index(d)

        def step(c, carry):
            outgoing[bases[d] + c] = padded[lists[row, c]]
            return carry

        lax.fori_loop(first, last, step, 0)

    for n in range(len(pieces) + 1):
        if n < len(pieces):
            guarded(pieces[n][3], functools.partial(gather, n))
        if n > 0:
            guarded(pieces[n - 1][3], lambda n=n: copy_of(n - 1).start())
    for n in range(len(pieces)):
        guarded(pieces[n][3], lambda n=n: copy_of(n).wait())


def exchange(lists, field, before, after, lats, lons, caps, bases, received, collective_id):
    tile = field.shape[1:]
    padded_rows = field.shape[0] + 2 * RLAT
    count = 2 * len(OFFSETS)
    return pl.pallas_call(
        functools.partial(exchange_kernel, lats, lons, caps, bases),
        out_shape=jax.ShapeDtypeStruct((received,) + tile, field.dtype),
        in_specs=[SMEM, ANY, ANY, ANY],
        out_specs=ANY,
        scratch_shapes=[
            pltpu.VMEM((padded_rows,) + tile, field.dtype),
            pltpu.VMEM((received,) + tile, field.dtype),
            pltpu.SemaphoreType.DMA((3,)),
            pltpu.SemaphoreType.DMA((count,)),
            pltpu.SemaphoreType.DMA((count,)),
        ],
        compiler_params=pltpu.CompilerParams(collective_id=collective_id, has_side_effects=True),
        name="exchange",
    )(lists, field, before, after)


def advect_kernel(step_rows, slots, code, table, counts, area, weights, field, before, after, recv, out, delta, src, gap, sem):
    g = pl.program_id(0)
    rows = field.shape[0]
    padded_rows = rows + 2 * RLAT
    received = recv.shape[0]

    @pl.when(g == 0)
    def _():
        loads = [
            pltpu.make_async_copy(before, src.at[pl.ds(0, RLAT)], sem.at[0]),
            pltpu.make_async_copy(field, src.at[pl.ds(RLAT, rows)], sem.at[1]),
            pltpu.make_async_copy(after, src.at[pl.ds(RLAT + rows, RLAT)], sem.at[2]),
            pltpu.make_async_copy(recv, src.at[pl.ds(padded_rows, received)], sem.at[3]),
        ]
        for load in loads:
            load.start()
        src[padded_rows + received] = jnp.zeros(src.shape[1:], src.dtype)
        gap[...] = jnp.zeros_like(gap)
        for load in loads:
            load.wait()

    together = 4 if step_rows % 4 == 0 else 1
    for first in range(0, step_rows, together):
        group = range(first, first + together)
        used = counts[g * step_rows + first]
        for tt in group[1:]:
            used = jnp.maximum(used, counts[g * step_rows + tt])
        for last in range(2, slots + 2, 2):
            width = min(last, slots)

            @pl.when((used > last - 2) & (used <= last))
            def _(group=group, width=width):
                total = gap[...]
                for tt in group:
                    t = g * step_rows + tt
                    left = jnp.concatenate([src[table[code[k, t]]] for k in range(width)], axis=1)
                    right = jnp.concatenate([weights[tt, 0, k] for k in range(width)], axis=1)
                    value = lax.dot_general(
                        left, right, (((1,), (1,)), ((), ())), preferred_element_type=jnp.float32
                    )
                    out[tt] = value
                    total += area[t] * (src[RLAT + t].astype(jnp.float32) - value)
                gap[...] = total

    @pl.when(g == pl.num_programs(0) - 1)
    def _():
        delta[...] = jnp.sum(gap[...].T, axis=0, keepdims=True)


def advect(code, table, counts, area, weights, field, before, after, recv):
    rows, channels, width = field.shape
    slots = weights.shape[2]
    step_rows = 8
    while rows % step_rows:
        step_rows -= 1
    sources = rows + 2 * RLAT + recv.shape[0] + 1
    block = (step_rows,) + weights.shape[1:]
    return pl.pallas_call(
        functools.partial(advect_kernel, step_rows, slots),
        grid=(rows // step_rows,),
        out_shape=(
            jax.ShapeDtypeStruct(field.shape, jnp.float32),
            jax.ShapeDtypeStruct((1, channels), jnp.float32),
        ),
        in_specs=[
            SMEM,
            SMEM,
            SMEM,
            SMEM,
            pl.BlockSpec(block, lambda g: (g, 0, 0, 0, 0)),
            ANY,
            ANY,
            ANY,
            ANY,
        ],
        out_specs=(
            pl.BlockSpec((step_rows, channels, width), lambda g: (g, 0, 0)),
            pl.BlockSpec((1, channels), lambda g: (0, 0)),
        ),
        scratch_shapes=[
            pltpu.VMEM((sources, channels, width), field.dtype),
            pltpu.VMEM((channels, width), jnp.float32),
            pltpu.SemaphoreType.DMA((4,)),
        ],
        compiler_params=pltpu.CompilerParams(dimension_semantics=("arbitrary",)),
        name="advect",
    )(code, table, counts, area, weights, field, before, after, recv)


def dense(field, before, after, weights, local_row, relative, active, area):
    padded = jnp.concatenate([before, field, after], axis=0)
    stack = jnp.stack(
        [padded if d == 0 else shifted(padded, "lon", -d) for d in range(-REACH, REACH + 1)], axis=1
    )
    rows = jnp.clip(local_row, 0, padded.shape[0] - 1)
    picked = stack[rows, jnp.clip(relative + REACH, 0, 2 * REACH)]
    picked = jnp.where(active[:, :, None, None], picked, jnp.zeros((), picked.dtype))
    advected = jnp.einsum("tkij,ktcj->tci", weights[:, 0], picked, preferred_element_type=jnp.float32)
    gap = jnp.sum(area[:, None, None] * (field.astype(jnp.float32) - advected), axis=(0, 2))
    return advected, gap[None, :]


def local(tracers, weights, source_row, source_block, slot_count):
    rows, width, levels, kinds = tracers.shape
    channels = levels * kinds
    lats, lons = lax.axis_size("lat"), lax.axis_size("lon")
    lat, lon = lax.axis_index("lat"), lax.axis_index("lon")
    field = tracers.reshape(rows, width, channels).transpose(0, 2, 1)
    slots = source_row.shape[2]
    table = area_table(rows * lats)
    total_area = float(width * lons * np.sum(table.astype(np.float64)))
    area = lax.dynamic_slice(jnp.asarray(table), (lat * rows,), (rows,))

    padded_rows = rows + 2 * RLAT
    lanes = -(-padded_rows // 128) * 128
    local_row = source_row[:, 0, :].T - (lat * rows - RLAT)
    relative = (source_block[:, 0, :].T - lon + REACH) % lons - REACH
    active = jnp.arange(slots, dtype=jnp.int32)[:, None] < slot_count[:, 0][None, :]
    away, own, unused = len(OFFSETS), len(OFFSETS), len(OFFSETS) + 1
    which = jnp.where(relative < 0, relative + REACH, relative + REACH - 1)
    which = jnp.where(relative == 0, own, which)
    code = jnp.where(active, which * lanes + local_row, unused * lanes)
    ids = jnp.arange(8 * lanes, dtype=jnp.int32)
    hit = (code.reshape(-1)[None, :] == ids[:, None]) & (ids < away * lanes)[:, None]
    need = jnp.any(hit, axis=1).astype(jnp.float32).reshape(8, lanes).astype(jnp.bfloat16)

    needs, before, after = share_needs(need, field, lats, lons)

    plans = [capacities(padded_rows, tier) for tier in TIERS]
    counted = jnp.sum(needs.astype(jnp.float32), axis=2)
    level = jnp.int32(0)
    for caps in plans:
        limit = np.zeros((lats, lons, 8), np.float32)
        for n, d in enumerate(OFFSETS):
            limit[:, :, n] = caps[d][1]
            limit[0, :, n] = limit[-1, :, n] = caps[d][0]
        over = jnp.any(counted > jnp.asarray(limit.reshape(lats * lons, 8)))
        level += over.astype(jnp.int32)

    upto = (jnp.arange(lanes)[:, None] <= jnp.arange(lanes)[None, :]).astype(jnp.float32)

    def ranks(mask):
        mask = mask.astype(jnp.float32)
        return jnp.sum(mask[:, :, None] * upto[None], axis=1).astype(jnp.int32) - 1

    def fast(n, field, before, after, weights, needs):
        caps = plans[n]
        bases, received = layout_of(caps)
        band = lax.dynamic_slice(needs, (lat * lons, 0, 0), (lons, 8, lanes))
        offsets = np.zeros((8,), np.int32)
        offsets[: len(OFFSETS)] = OFFSETS
        dest = (lon - jnp.asarray(offsets)) % lons
        chosen = jnp.arange(lons, dtype=jnp.int32)[:, None] == dest[None, :]
        wanted = jnp.sum(jnp.where(chosen[:, :, None], band.astype(jnp.float32), 0.0), axis=0)
        rank = jnp.where(wanted > 0, ranks(wanted), -1)
        place = jnp.arange(lanes, dtype=jnp.int32)
        match = rank[:, :, None] == place[None, None, :]
        lists = jnp.sum(jnp.where(match, place[None, :, None], 0), axis=1)
        recv = exchange(lists, field, before, after, lats, lons, caps, bases, received, 2 + n)
        start = np.zeros((8, 1), np.int32)
        start[:away, 0] = [bases[d] + padded_rows for d in OFFSETS]
        kind = jnp.arange(8, dtype=jnp.int32)[:, None]
        spot = jnp.where(kind == own, place[None, :], padded_rows + received)
        spot = jnp.where(kind < away, ranks(need) + jnp.asarray(start), spot)
        return advect(code, spot.reshape(-1), slot_count[:, 0], area, weights, field, before, after, recv)

    def general(field, before, after, weights, needs):
        return dense(field, before, after, weights, local_row, relative, active, area)

    paths = [functools.partial(fast, n) for n in range(len(plans))] + [general]
    advected, delta = lax.switch(level, paths, field, before, after, weights, needs)
    total = sum_over_devices(delta, lats, lons)
    fixed = advected + (total[0] / total_area)[None, :, None]
    return fixed.transpose(0, 2, 1).reshape(rows, width, levels, kinds)


def solution(mesh):
    return jax.shard_map(
        local,
        mesh=mesh,
        in_specs=(
            P("lat", "lon", None, None),
            P("lat", "lon", None, None, None),
            P("lat", "lon", None),
            P("lat", "lon", None),
            P("lat", "lon"),
        ),
        out_specs=P("lat", "lon", None, None),
        check_vma=False,
    )
```

```python
import functools
import math

import jax
import jax.numpy as jnp
import numpy as np
from jax import lax
from jax.experimental import pallas as pl
from jax.experimental.pallas import tpu as pltpu
from jax.sharding import PartitionSpec as P

RLAT = 4
REACH = 3
OFFSETS = tuple(d for d in range(-REACH, REACH + 1) if d != 0)
MESH = pl.DeviceIdType.MESH
ANY = pl.BlockSpec(memory_space=pl.ANY)
VMEM = pl.BlockSpec(memory_space=pltpu.VMEM)
SMEM = pl.BlockSpec(memory_space=pltpu.SMEM)


def shifted(value, axis, by):
    length = lax.axis_size(axis)
    return lax.ppermute(value, axis, [(i, (i + by) % length) for i in range(length)])


def area_table(total_rows):
    angle = -0.5 * math.pi + (np.arange(total_rows) + 0.5) * (math.pi / total_rows)
    return np.cos(angle).astype(np.float32)


def everyone(lats, lons):
    return [(a, b) for a in range(lats) for b in range(lons) if (a, b) != (0, 0)]


def send_to_all(lats, lons, mine, slots, send_sem, recv_sem):
    lat, lon = lax.axis_index("lat"), lax.axis_index("lon")
    me = lat * lons + lon
    copies = []
    for n, (a, b) in enumerate(everyone(lats, lons)):
        peer = (lax.rem(lat + a, lats), lax.rem(lon + b, lons))
        copy = pltpu.make_async_remote_copy(
            src_ref=mine,
            dst_ref=slots.at[me],
            send_sem=send_sem.at[n],
            recv_sem=recv_sem.at[n],
            device_id=peer,
            device_id_type=MESH,
        )
        copy.start()
        copies.append(copy)
    return copies


def greet(lats, lons):
    lat, lon = lax.axis_index("lat"), lax.axis_index("lon")
    barrier = pltpu.get_barrier_semaphore()
    peers = everyone(lats, lons)
    for a, b in peers:
        peer = (lax.rem(lat + a, lats), lax.rem(lon + b, lons))
        pl.semaphore_signal(barrier, inc=1, device_id=peer, device_id_type=MESH)
    pl.semaphore_wait(barrier, len(peers))


def needs_kernel(lats, lons, need, field, slots, before, after, send_sem, recv_sem, halo_send, halo_recv):
    lat, lon = lax.axis_index("lat"), lax.axis_index("lon")
    rows = field.shape[0]
    greet(lats, lons)

    def up():
        return pltpu.make_async_remote_copy(
            src_ref=field.at[pl.ds(rows - RLAT, RLAT)],
            dst_ref=before,
            send_sem=halo_send.at[0],
            recv_sem=halo_recv.at[0],
            device_id=(lax.rem(lat + 1, lats), lon),
            device_id_type=MESH,
        )

    def down():
        return pltpu.make_async_remote_copy(
            src_ref=field.at[pl.ds(0, RLAT)],
            dst_ref=after,
            send_sem=halo_send.at[1],
            recv_sem=halo_recv.at[1],
            device_id=(lax.rem(lat + lats - 1, lats), lon),
            device_id_type=MESH,
        )

    up().start()
    down().start()
    copies = send_to_all(lats, lons, need, slots, send_sem, recv_sem)
    slots[lat * lons + lon] = need[...]
    for copy in copies:
        copy.wait()
    up().wait()
    down().wait()


def share_needs(need, field, lats, lons):
    count = lats * lons
    halo = jax.ShapeDtypeStruct((RLAT,) + field.shape[1:], field.dtype)
    return pl.pallas_call(
        functools.partial(needs_kernel, lats, lons),
        out_shape=(jax.ShapeDtypeStruct((count,) + need.shape, need.dtype), halo, halo),
        in_specs=[VMEM, ANY],
        out_specs=(VMEM, ANY, ANY),
        scratch_shapes=[
            pltpu.SemaphoreType.DMA((count - 1,)),
            pltpu.SemaphoreType.DMA((count - 1,)),
            pltpu.SemaphoreType.DMA((2,)),
            pltpu.SemaphoreType.DMA((2,)),
        ],
        compiler_params=pltpu.CompilerParams(collective_id=0, has_side_effects=True),
        name="share_needs",
    )(need, field)


def total_kernel(lats, lons, part, total, slots, send_sem, recv_sem):
    greet(lats, lons)
    copies = send_to_all(lats, lons, part, slots, send_sem, recv_sem)
    slots[lax.axis_index("lat") * lons + lax.axis_index("lon")] = part[...]
    for copy in copies:
        copy.wait()
    total[...] = jnp.sum(slots[...], axis=0)


def sum_over_devices(part, lats, lons):
    count = lats * lons
    return pl.pallas_call(
        functools.partial(total_kernel, lats, lons),
        out_shape=jax.ShapeDtypeStruct(part.shape, part.dtype),
        in_specs=[VMEM],
        out_specs=VMEM,
        scratch_shapes=[
            pltpu.VMEM((count,) + part.shape, part.dtype),
            pltpu.SemaphoreType.DMA((count - 1,)),
            pltpu.SemaphoreType.DMA((count - 1,)),
        ],
        compiler_params=pltpu.CompilerParams(collective_id=1, has_side_effects=True),
        name="sum_masses",
    )(part)


TIERS = ((50, 42, 37, 3), (52, 44, 39, 4), (54, 46, 41, 4), (60, 52, 46, 5))


def capacities(padded_rows, tier):
    near_polar, near_inner, far_polar = [padded_rows * part // 72 for part in tier[:3]]
    by_reach = {1: (near_polar, near_inner), 2: (far_polar, 0)}
    return {d: by_reach.get(abs(d), (tier[3], 0)) for d in OFFSETS}


def layout_of(caps):
    bases, received = {}, 0
    for d in OFFSETS:
        bases[d] = received
        received += max(caps[d])
    return bases, received


def exchange_kernel(
    lats, lons, caps, bases, lists, field, before, after, recv, padded, outgoing, load_sem, send_sem, recv_sem
):
    lat, lon = lax.axis_index("lat"), lax.axis_index("lon")
    rows = field.shape[0]
    loads = [
        pltpu.make_async_copy(before, padded.at[pl.ds(0, RLAT)], load_sem.at[0]),
        pltpu.make_async_copy(field, padded.at[pl.ds(RLAT, rows)], load_sem.at[1]),
        pltpu.make_async_copy(after, padded.at[pl.ds(RLAT + rows, RLAT)], load_sem.at[2]),
    ]
    for load in loads:
        load.start()
    barrier = pltpu.get_barrier_semaphore()
    for d in OFFSETS:
        peer = (lat, lax.rem(lon + lons - d, lons))
        pl.semaphore_signal(barrier, inc=1, device_id=peer, device_id_type=MESH)
    pl.semaphore_wait(barrier, len(OFFSETS))
    for load in loads:
        load.wait()

    polar = (lat == 0) | (lat == lats - 1)
    pieces = []
    for d in sorted(OFFSETS, key=lambda d: (abs(d), d)):
        outer, inner = caps[d]
        if inner:
            pieces.append((d, 0, inner, False))
    for d in sorted(OFFSETS, key=lambda d: (abs(d) == 1, abs(d), d)):
        outer, inner = caps[d]
        if outer > inner:
            pieces.append((d, inner, outer, True))

    def guarded(only_polar, act):
        if only_polar:
            pl.when(polar)(act)
        else:
            act()

    def copy_of(n):
        d, first, last, _ = pieces[n]
        span = pl.ds(bases[d] + first, last - first)
        return pltpu.make_async_remote_copy(
            src_ref=outgoing.at[span],
            dst_ref=recv.at[span],
            send_sem=send_sem.at[n],
            recv_sem=recv_sem.at[n],
            device_id=(lat, lax.rem(lon + lons - d, lons)),
            device_id_type=MESH,
        )

    def gather(n):
        d, first, last, _ = pieces[n]
        row = OFFSETS.index(d)

        def step(c, carry):
            outgoing[bases[d] + c] = padded[lists[row, c]]
            return carry

        lax.fori_loop(first, last, step, 0)

    for n in range(len(pieces) + 1):
        if n < len(pieces):
            guarded(pieces[n][3], functools.partial(gather, n))
        if n > 0:
            guarded(pieces[n - 1][3], lambda n=n: copy_of(n - 1).start())
    for n in range(len(pieces)):
        guarded(pieces[n][3], lambda n=n: copy_of(n).wait())


def exchange(lists, field, before, after, lats, lons, caps, bases, received, collective_id):
    tile = field.shape[1:]
    padded_rows = field.shape[0] + 2 * RLAT
    count = 2 * len(OFFSETS)
    return pl.pallas_call(
        functools.partial(exchange_kernel, lats, lons, caps, bases),
        out_shape=jax.ShapeDtypeStruct((received,) + tile, field.dtype),
        in_specs=[SMEM, ANY, ANY, ANY],
        out_specs=ANY,
        scratch_shapes=[
            pltpu.VMEM((padded_rows,) + tile, field.dtype),
            pltpu.VMEM((received,) + tile, field.dtype),
            pltpu.SemaphoreType.DMA((3,)),
            pltpu.SemaphoreType.DMA((count,)),
            pltpu.SemaphoreType.DMA((count,)),
        ],
        compiler_params=pltpu.CompilerParams(collective_id=collective_id, has_side_effects=True),
        name="exchange",
    )(lists, field, before, after)


def advect_kernel(step_rows, slots, code, table, counts, area, weights, field, before, after, recv, out, delta, src, gap, sem):
    g = pl.program_id(0)
    rows = field.shape[0]
    padded_rows = rows + 2 * RLAT
    received = recv.shape[0]

    @pl.when(g == 0)
    def _():
        loads = [
            pltpu.make_async_copy(before, src.at[pl.ds(0, RLAT)], sem.at[0]),
            pltpu.make_async_copy(field, src.at[pl.ds(RLAT, rows)], sem.at[1]),
            pltpu.make_async_copy(after, src.at[pl.ds(RLAT + rows, RLAT)], sem.at[2]),
            pltpu.make_async_copy(recv, src.at[pl.ds(padded_rows, received)], sem.at[3]),
        ]
        for load in loads:
            load.start()
        src[padded_rows + received] = jnp.zeros(src.shape[1:], src.dtype)
        gap[...] = jnp.zeros_like(gap)
        for load in loads:
            load.wait()

    together = 4 if step_rows % 4 == 0 else 1
    for first in range(0, step_rows, together):
        group = range(first, first + together)
        used = counts[g * step_rows + first]
        for tt in group[1:]:
            used = jnp.maximum(used, counts[g * step_rows + tt])
        for last in range(2, slots + 2, 2):
            width = min(last, slots)

            @pl.when((used > last - 2) & (used <= last))
            def _(group=group, width=width):
                total = gap[...]
                for tt in group:
                    t = g * step_rows + tt
                    left = jnp.concatenate([src[table[code[k, t]]] for k in range(width)], axis=1)
                    right = jnp.concatenate([weights[tt, 0, k] for k in range(width)], axis=1)
                    value = lax.dot_general(
                        left, right, (((1,), (1,)), ((), ())), preferred_element_type=jnp.float32
                    )
                    out[tt] = value
                    total += area[t] * (src[RLAT + t].astype(jnp.float32) - value)
                gap[...] = total

    @pl.when(g == pl.num_programs(0) - 1)
    def _():
        delta[...] = jnp.sum(gap[...].T, axis=0, keepdims=True)


def advect(code, table, counts, area, weights, field, before, after, recv):
    rows, channels, width = field.shape
    slots = weights.shape[2]
    step_rows = 8
    while rows % step_rows:
        step_rows -= 1
    sources = rows + 2 * RLAT + recv.shape[0] + 1
    block = (step_rows,) + weights.shape[1:]
    return pl.pallas_call(
        functools.partial(advect_kernel, step_rows, slots),
        grid=(rows // step_rows,),
        out_shape=(
            jax.ShapeDtypeStruct(field.shape, jnp.float32),
            jax.ShapeDtypeStruct((1, channels), jnp.float32),
        ),
        in_specs=[
            SMEM,
            SMEM,
            SMEM,
            SMEM,
            pl.BlockSpec(block, lambda g: (g, 0, 0, 0, 0)),
            ANY,
            ANY,
            ANY,
            ANY,
        ],
        out_specs=(
            pl.BlockSpec((step_rows, channels, width), lambda g: (g, 0, 0)),
            pl.BlockSpec((1, channels), lambda g: (0, 0)),
        ),
        scratch_shapes=[
            pltpu.VMEM((sources, channels, width), field.dtype),
            pltpu.VMEM((channels, width), jnp.float32),
            pltpu.SemaphoreType.DMA((4,)),
        ],
        compiler_params=pltpu.CompilerParams(dimension_semantics=("arbitrary",)),
        name="advect",
    )(code, table, counts, area, weights, field, before, after, recv)


def dense(field, before, after, weights, local_row, relative, active, area):
    padded = jnp.concatenate([before, field, after], axis=0)
    stack = jnp.stack(
        [padded if d == 0 else shifted(padded, "lon", -d) for d in range(-REACH, REACH + 1)], axis=1
    )
    rows = jnp.clip(local_row, 0, padded.shape[0] - 1)
    picked = stack[rows, jnp.clip(relative + REACH, 0, 2 * REACH)]
    picked = jnp.where(active[:, :, None, None], picked, jnp.zeros((), picked.dtype))
    advected = jnp.einsum("tkij,ktcj->tci", weights[:, 0], picked, preferred_element_type=jnp.float32)
    gap = jnp.sum(area[:, None, None] * (field.astype(jnp.float32) - advected), axis=(0, 2))
    return advected, gap[None, :]


def local(tracers, weights, source_row, source_block, slot_count):
    rows, width, levels, kinds = tracers.shape
    channels = levels * kinds
    lats, lons = lax.axis_size("lat"), lax.axis_size("lon")
    lat, lon = lax.axis_index("lat"), lax.axis_index("lon")
    field = tracers.reshape(rows, width, channels).transpose(0, 2, 1)
    slots = source_row.shape[2]
    table = area_table(rows * lats)
    total_area = float(width * lons * np.sum(table.astype(np.float64)))
    area = lax.dynamic_slice(jnp.asarray(table), (lat * rows,), (rows,))

    padded_rows = rows + 2 * RLAT
    lanes = -(-padded_rows // 128) * 128
    local_row = source_row[:, 0, :].T - (lat * rows - RLAT)
    relative = (source_block[:, 0, :].T - lon + REACH) % lons - REACH
    active = jnp.arange(slots, dtype=jnp.int32)[:, None] < slot_count[:, 0][None, :]
    away, own, unused = len(OFFSETS), len(OFFSETS), len(OFFSETS) + 1
    which = jnp.where(relative < 0, relative + REACH, relative + REACH - 1)
    which = jnp.where(relative == 0, own, which)
    code = jnp.where(active, which * lanes + local_row, unused * lanes)
    ids = jnp.arange(8 * lanes, dtype=jnp.int32)
    hit = (code.reshape(-1)[None, :] == ids[:, None]) & (ids < away * lanes)[:, None]
    need = jnp.any(hit, axis=1).astype(jnp.float32).reshape(8, lanes).astype(jnp.bfloat16)

    needs, before, after = share_needs(need, field, lats, lons)

    plans = [capacities(padded_rows, tier) for tier in TIERS]
    counted = jnp.sum(needs.astype(jnp.float32), axis=2)
    level = jnp.int32(0)
    for caps in plans:
        limit = np.zeros((lats, lons, 8), np.float32)
        for n, d in enumerate(OFFSETS):
            limit[:, :, n] = caps[d][1]
            limit[0, :, n] = limit[-1, :, n] = caps[d][0]
        over = jnp.any(counted > jnp.asarray(limit.reshape(lats * lons, 8)))
        level += over.astype(jnp.int32)

    upto = (jnp.arange(lanes)[:, None] <= jnp.arange(lanes)[None, :]).astype(jnp.float32)

    def ranks(mask):
        mask = mask.astype(jnp.float32)
        return jnp.sum(mask[:, :, None] * upto[None], axis=1).astype(jnp.int32) - 1

    def fast(n, field, before, after, weights, needs):
        caps = plans[n]
        bases, received = layout_of(caps)
        band = lax.dynamic_slice(needs, (lat * lons, 0, 0), (lons, 8, lanes))
        offsets = np.zeros((8,), np.int32)
        offsets[: len(OFFSETS)] = OFFSETS
        dest = (lon - jnp.asarray(offsets)) % lons
        chosen = jnp.arange(lons, dtype=jnp.int32)[:, None] == dest[None, :]
        wanted = jnp.sum(jnp.where(chosen[:, :, None], band.astype(jnp.float32), 0.0), axis=0)
        rank = jnp.where(wanted > 0, ranks(wanted), -1)
        place = jnp.arange(lanes, dtype=jnp.int32)
        match = rank[:, :, None] == place[None, None, :]
        lists = jnp.sum(jnp.where(match, place[None, :, None], 0), axis=1)
        recv = exchange(lists, field, before, after, lats, lons, caps, bases, received, 2 + n)
        start = np.zeros((8, 1), np.int32)
        start[:away, 0] = [bases[d] + padded_rows for d in OFFSETS]
        kind = jnp.arange(8, dtype=jnp.int32)[:, None]
        spot = jnp.where(kind == own, place[None, :], padded_rows + received)
        spot = jnp.where(kind < away, ranks(need) + jnp.asarray(start), spot)
        return advect(code, spot.reshape(-1), slot_count[:, 0], area, weights, field, before, after, recv)

    def general(field, before, after, weights, needs):
        return dense(field, before, after, weights, local_row, relative, active, area)

    paths = [functools.partial(fast, n) for n in range(len(plans))] + [general]
    advected, delta = lax.switch(level, paths, field, before, after, weights, needs)
    total = sum_over_devices(delta, lats, lons)
    fixed = advected + (total[0] / total_area)[None, :, None]
    return fixed.transpose(0, 2, 1).reshape(rows, width, levels, kinds)


def solution(mesh):
    return jax.shard_map(
        local,
        mesh=mesh,
        in_specs=(
            P("lat", "lon", None, None),
            P("lat", "lon", None, None, None),
            P("lat", "lon", None),
            P("lat", "lon", None),
            P("lat", "lon"),
        ),
        out_specs=P("lat", "lon", None, None),
        check_vma=False,
    )
```
